32 devices in a mesh: groups: 2 (over y), dp: 4 (over x, core), tp: 4 (over z).
Axes of the slice: x: 2, y: 2, z: 4, core: 2. Of those that a mesh axis runs over, the one named last changes fastest.
Arguments:
- tokens: bfloat16 [256, 6144], P(('groups', 'tp'), 'dp'), parts along dimension 0, may hold values from -6 to 6
- gate_weight: bfloat16 [6144, 16384], P('dp', 'tp'), may hold values from -0.078125 to 0.078125
- up_weight: bfloat16 [6144, 16384], P('dp', 'tp'), may hold values from -0.078125 to 0.078125
- down_weight: bfloat16 [16384, 6144], P('tp', 'dp'), may hold values from -0.046875 to 0.046875
- expert_ids: int32 [256, 2], P(('groups', 'tp')), parts along dimension 0, may hold values from 0 to 7, as said below
- route_weights: float32 [256, 2], P(('groups', 'tp')), parts along dimension 0, may hold values from 0.1 to 1
Outputs:
- mixed: bfloat16 [256, 6144], P(('groups', 'tp'), 'dp'), parts along dimension 0
The draws below stay inside these ranges and needn't reach their ends.
There are 2 independent parts, one for each index of `groups`. The reference program is written for one: setup_inputs(seed, part) draws one part's arguments, and reference() takes and returns one part's arrays. A program takes and returns all parts, laid end to end along the dimension named above; an argument that names none is the same for every part. Nothing has to cross between parts.
Inputs may be any that keep to these rules, and one draw needn't show every extreme that they name: `expert_ids`: each row names two different experts. Among the 32 rows of one index of tp, expert 0 is named by 1 to 16 rows, and by exactly 16 rows on at least one index of tp.
All inputs are finite; a program needn't handle non-finite values.
Results may differ from the reference program's by a relative error of at most 0.03.
Values may be sent and summed in bfloat16 or wider, within the bound.
No kernel may reach another device: no remote copies, remote signals or barrier semaphores. Data moves between devices by JAX's collectives and lax.ppermute only.
A program may use at most 64 MiB of HBM per device.

```python
import jax
import jax.numpy as jnp
from jax import lax

D = 6144
FF = 16384
EXPERTS = 8
TOK_TP = 32
TOKENS = 128
MOST = 16
N_DP = 4


def draw_expert_ids(key, part):
    blocks = TOKENS // TOK_TP
    subkeys = jax.random.split(key, 6)
    counts = jax.random.randint(subkeys[0], (blocks,), 1, MOST + 1)
    forced = jax.random.randint(subkeys[1], (), 0, blocks)
    counts = jnp.where(jnp.arange(blocks) == forced, MOST, counts)

    def shuffle(subkey):
        return jax.random.permutation(subkey, TOK_TP)
    shuffles = jax.vmap(shuffle)(jax.random.split(subkeys[2], blocks))
    positions = jnp.argsort(shuffles, axis=1)
    routed = (positions < counts[:, None]).reshape(TOKENS)
    primary = jax.random.randint(subkeys[3], (TOKENS,), 1, EXPERTS)
    spare_id = jax.random.randint(subkeys[4], (TOKENS,), 1, EXPERTS - 1)
    secondary = spare_id + (spare_id >= primary).astype(jnp.int32)
    placing = jax.random.randint(subkeys[5], (TOKENS,), 0, 2)
    slot_one = jnp.where(routed, jnp.where(placing == 0, 0, primary), primary)
    slot_two = jnp.where(routed, jnp.where(placing == 0, primary, 0), secondary)
    return jnp.stack([slot_one, slot_two], axis=1).astype(jnp.int32)


def levels(stream_key, shape, shards, least, top_value):
    level, own = 1.0, jax.random.fold_in(stream_key, 6)
    for position, blocks in shards:
        steps = jnp.exp(jax.random.uniform(jax.random.fold_in(own, position), (blocks,), jnp.float32, least / len(shards), top_value / len(shards)))
        level = level * jnp.repeat(steps, shape[position] // blocks).reshape([-1 if axis == position else 1 for axis in range(len(shape))])
    return level


def bell_draw(own_key, extent, deviation, most, cuts=(), kind=jnp.bfloat16):
    values = deviation * jax.random.normal(own_key, extent, jnp.float32)
    if cuts:
        values = values * levels(own_key, extent, cuts, -0.22, 0.18)
    return jnp.clip(values, -most, most).astype(kind)


def setup_inputs(seed: int = 0, part: int = 0) -> dict:
    key_list = jax.random.split(jax.random.key(seed), 7)
    part_splits = jax.random.split(jax.random.fold_in(key_list[6], part), 7)
    return {
        "tokens": bell_draw(part_splits[0], (TOKENS, D), 1.0, 6.0, ((0, 4), (1, 4))),
        "gate_weight": bell_draw(key_list[1], (D, FF), D ** -0.5, 0.078125, ((0, 4), (1, 4))),
        "up_weight": bell_draw(key_list[2], (D, FF), D ** -0.5, 0.078125, ((0, 4), (1, 4))),
        "down_weight": bell_draw(key_list[3], (FF, D), FF ** -0.5, 0.046875, ((0, 4), (1, 4))),
        "expert_ids": draw_expert_ids(jax.random.fold_in(jax.random.fold_in(key_list[6], part), 71), part),
        "route_weights": jnp.clip(0.1 + 0.9 * jax.random.uniform(part_splits[5], (TOKENS, 2), jnp.float32) ** levels(part_splits[5], (TOKENS, 2), ((0, 4),), -0.2, 0.2), 0.1, 1.0),
    }


def reference(tokens, gate_weight, up_weight, down_weight, expert_ids, route_weights):
    slice_width = D // N_DP
    token_slices = tokens.reshape(TOKENS, N_DP, slice_width).transpose(1, 0, 2)
    gate_slices = gate_weight.reshape(N_DP, slice_width, FF)
    up_slices = up_weight.reshape(N_DP, slice_width, FF)

    def accumulate(carried, inputs):
        token_part, gate_part, up_part = inputs
        gate_term = jnp.dot(token_part, gate_part, preferred_element_type=jnp.float32).astype(jnp.bfloat16)
        up_term = jnp.dot(token_part, up_part, preferred_element_type=jnp.float32).astype(jnp.bfloat16)
        return (carried[0] + gate_term.astype(jnp.float32), carried[1] + up_term.astype(jnp.float32)), None

    zeros_start = jnp.zeros((TOKENS, FF), jnp.float32)
    (gate, up), _ = lax.scan(accumulate, (zeros_start, zeros_start), (token_slices, gate_slices, up_slices))
    hidden = (jax.nn.silu(gate) * up).astype(jnp.bfloat16)
    expert_out = jnp.dot(hidden, down_weight, preferred_element_type=jnp.float32)
    combine = jnp.sum(jnp.where(expert_ids == 0, route_weights, jnp.zeros_like(route_weights)), axis=1)
    return (combine[:, None] * expert_out).astype(jnp.bfloat16)
```

```python
import functools

import jax
import jax.numpy as jnp
from jax import lax
from jax.experimental import pallas as pl
from jax.experimental.pallas import tpu as pltpu
from jax.sharding import PartitionSpec as P

MOST = 16
F32 = jnp.float32
BF16 = jnp.bfloat16
PRIOR = 10000
WIDE = 512
GRANT = 8 * 1024 * 1024
VM = pl.BlockSpec(memory_space=pltpu.VMEM)


def call(body, outs, flops, nbytes, *args, scratch=()):
    return pl.pallas_call(
        body,
        out_shape=outs,
        in_specs=[VM] * len(args),
        out_specs=jax.tree.map(lambda _: VM, outs),
        scratch_shapes=scratch,
        compiler_params=pltpu.CompilerParams(vmem_limit_bytes=GRANT),
        cost_estimate=pl.CostEstimate(flops=flops, bytes_accessed=nbytes, transcendentals=0),
    )(*args)


def shape(dims, dtype):
    return jax.ShapeDtypeStruct(dims, dtype)


def in_vmem(array):
    return pltpu.with_memory_space_constraint(array, pltpu.VMEM)


def slots(ids_t):
    count = ids_t.shape[1]
    held = jnp.max(jnp.where(ids_t == 0, 1.0, 0.0), axis=0, keepdims=True)
    row = lax.broadcasted_iota(jnp.int32, (count, count), 0)
    col = lax.broadcasted_iota(jnp.int32, (count, count), 1)
    spread = jnp.broadcast_to(held, (count, count))
    rank = jnp.sum(jnp.where(col < row, spread, 0.0), axis=1, keepdims=True)
    routed = jnp.sum(jnp.where(col == row, spread, 0.0), axis=1, keepdims=True)
    slot = lax.broadcasted_iota(jnp.int32, (count, MOST), 1).astype(F32)
    return jnp.where((slot == rank) & (routed > 0.0), 1.0, 0.0)


def pack_body(ids_ref, tokens_ref, out_ref):
    one_hot = slots(ids_ref[...]).astype(BF16)
    out_ref[...] = lax.dot_general(
        one_hot, tokens_ref[...], (((0,), (0,)), ((), ())), preferred_element_type=F32
    ).astype(BF16)


def gate_up_body(n_tp, *refs):
    blocks = refs[:n_tp]
    gate_ref, up_ref, keep_ref, send_ref, scratch = refs[n_tp:]
    place = lax.axis_index("dp") ^ lax.axis_index("tp")
    for q, block in enumerate(blocks):
        spot = place ^ q
        spot = (spot % 2) * 2 + spot // 2
        scratch[pl.ds(pl.multiple_of(spot * MOST, MOST), MOST), :] = block[...]
    rows = scratch[...]
    half = rows.shape[0] // 2
    width = gate_ref.shape[1]
    step = min(WIDE, width)
    for k, weight in enumerate((gate_ref, up_ref)):

        def chunk(i, _, k=k, weight=weight):
            at = pl.ds(pl.multiple_of(i * step, step), step)
            part = jnp.dot(rows, weight[:, at], preferred_element_type=F32).astype(BF16)
            keep_ref[k, :, at] = part[:half]
            send_ref[k, :, at] = part[half:]
            return 0

        lax.fori_loop(0, width // step, chunk, 0)


def fold_body(keep_ref, got_ref, own_ref, send_ref):
    half = keep_ref.shape[1] // 2
    own_ref[...] = keep_ref[:, :half].astype(F32) + got_ref[:, :half].astype(F32)
    send_ref[...] = (keep_ref[:, half:].astype(F32) + got_ref[:, half:].astype(F32)).astype(BF16)


def hidden_body(own_ref, got_ref, out_ref):
    total = own_ref[...] + got_ref[...].astype(F32)
    gate, up = total[0], total[1]
    out_ref[...] = (gate / (1.0 + jnp.exp(-gate)) * up).astype(BF16)


def down_body(n_tp, *refs):
    weight_ref, own_ref = refs[4:6]
    sends, scratch = refs[6 : 5 + n_tp], refs[5 + n_tp]
    hidden = jnp.concatenate([ref[...] for ref in refs[:4]], axis=0)
    width = weight_ref.shape[1]
    step = min(WIDE, width)

    def chunk(i, _):
        at = pl.ds(pl.multiple_of(i * step, step), step)
        scratch[:, at] = jnp.dot(hidden, weight_ref[:, at], preferred_element_type=F32)
        return 0

    lax.fori_loop(0, width // step, chunk, 0)
    place = lax.axis_index("dp") ^ lax.axis_index("tp")
    for q in range(n_tp):
        block = scratch[pl.ds(pl.multiple_of((place ^ q) * MOST, MOST), MOST), :]
        if q == 0:
            own_ref[...] = block
        else:
            sends[q - 1][...] = block.astype(BF16)


def final_body(ids_ref, route_ref, own_ref, *refs):
    out_ref = refs[-1]
    total = own_ref[...]
    for got in refs[:-1]:
        total = total + got[...].astype(F32)
    ids = ids_ref[...]
    count = ids.shape[1]
    held = jnp.sum(jnp.where(ids == 0, route_ref[...], 0.0), axis=0, keepdims=True)
    row = lax.broadcasted_iota(jnp.int32, (count, count), 0)
    col = lax.broadcasted_iota(jnp.int32, (count, count), 1)
    combine = jnp.sum(
        jnp.where(col == row, jnp.broadcast_to(held, (count, count)), 0.0), axis=1, keepdims=True
    )
    spread = jnp.dot(
        slots(ids), total, precision=lax.Precision.HIGHEST, preferred_element_type=F32
    )
    out_ref[...] = (combine * spread).astype(BF16)


def swap(value, axis, size, mask):
    return lax.ppermute(value, axis, [(i, i ^ mask) for i in range(size)])


def direct(n_dp, n_tp, tokens, gate_weight, up_weight, down_weight, expert_ids, route_weights):
    ids_t, route_t = expert_ids.T, route_weights.T
    model, width = gate_weight.shape
    out_width = down_weight.shape[1]
    total = MOST * n_tp
    gate_weight, up_weight, down_weight = map(in_vmem, (gate_weight, up_weight, down_weight))
    packed = call(
        pack_body, shape((MOST, model), BF16), PRIOR * total * model * width, PRIOR * model * width, ids_t, tokens
    )
    got = [packed] + [swap(packed, "tp", n_tp, q) for q in range(1, n_tp)]
    keep, send = call(
        functools.partial(gate_up_body, n_tp),
        [shape((2, total // 2, width), BF16)] * 2,
        4 * total * model * width,
        4 * model * width,
        *got,
        gate_weight,
        up_weight,
        scratch=[pltpu.VMEM((total, model), BF16)],
    )
    got = swap(send, "dp", n_dp, 1)
    own, send = call(
        fold_body,
        [shape((2, total // 4, width), F32), shape((2, total // 4, width), BF16)],
        total * width,
        6 * total * width,
        keep,
        got,
    )
    got = swap(send, "dp", n_dp, 2)
    hidden = call(
        hidden_body, shape((total // 4, width), BF16), total * width, 3 * total * width, own, got
    )
    across = swap(hidden, "dp", n_dp, 2)
    beside = swap(hidden, "dp", n_dp, 1)
    corner = swap(across, "dp", n_dp, 1)
    own, *sends = call(
        functools.partial(down_body, n_tp),
        [shape((MOST, out_width), F32)] + [shape((MOST, out_width), BF16)] * (n_tp - 1),
        2 * total * width * out_width,
        2 * width * out_width,
        hidden,
        beside,
        across,
        corner,
        down_weight,
        scratch=[pltpu.VMEM((total, out_width), F32)],
    )
    got = [swap(s, "tp", n_tp, q + 1) for q, s in enumerate(sends)]
    return call(
        final_body,
        shape((tokens.shape[0], out_width), BF16),
        2 * tokens.size,
        4 * tokens.size,
        ids_t,
        route_t,
        own,
        *got,
    )


def general(tokens, gate_weight, up_weight, down_weight, expert_ids, route_weights):
    held_mask = expert_ids == 0
    combine = jnp.sum(jnp.where(held_mask, route_weights, jnp.zeros_like(route_weights)), axis=1)
    hidden_width = gate_weight.shape[1]
    routed = jnp.any(held_mask, axis=1)
    slot_rank = jnp.cumsum(routed.astype(jnp.int32)) - 1
    slot_ids = jnp.arange(MOST, dtype=jnp.int32)
    dispatch = ((slot_rank[None, :] == slot_ids[:, None]) & routed[None, :]).astype(BF16)
    packed = jnp.dot(dispatch, tokens, preferred_element_type=F32).astype(BF16)
    row_block = lax.all_gather(packed, "tp", axis=0, tiled=True)
    gate_part = jnp.dot(row_block, gate_weight, preferred_element_type=F32).astype(BF16)
    up_part = jnp.dot(row_block, up_weight, preferred_element_type=F32).astype(BF16)
    gate_up = jnp.concatenate([gate_part, up_part], axis=1)
    summed = lax.psum(gate_up, "dp").astype(F32)
    hidden = (jax.nn.silu(summed[:, :hidden_width]) * summed[:, hidden_width:]).astype(BF16)
    partial_value = jnp.dot(hidden, down_weight, preferred_element_type=F32)
    result = jnp.dot(
        dispatch.T.astype(F32),
        lax.psum_scatter(
            partial_value.astype(BF16), "tp", scatter_dimension=0, tiled=True
        ).astype(F32),
        precision=lax.Precision.HIGHEST,
    )
    return (combine[:, None] * result).astype(BF16)


def solution(mesh):
    n_dp, n_tp = mesh.shape["dp"], mesh.shape["tp"]
    in_specs = (
        P(("groups", "tp"), "dp"),
        P("dp", "tp"),
        P("dp", "tp"),
        P("tp", "dp"),
        P(("groups", "tp"), None),
        P(("groups", "tp"), None),
    )
    out_specs = P(("groups", "tp"), "dp")
    body = functools.partial(direct, n_dp, n_tp) if n_dp == n_tp == 4 else general
    return jax.shard_map(body, mesh=mesh, in_specs=in_specs, out_specs=out_specs, check_vma=False)
```

```python
import functools

import jax
import jax.numpy as jnp
from jax import lax
from jax.experimental import pallas as pl
from jax.experimental.pallas import tpu as pltpu
from jax.sharding import PartitionSpec as P


MOST = 16
F32 = jnp.float32
BF16 = jnp.bfloat16
PRIOR = 100000
WIDE = 2048
CUTS = (0, 4, 8, 12, 16)
GRANT = 2 * 1024 * 1024
VM = pl.BlockSpec(memory_space=pltpu.VMEM)


def call(body, outs, flops, nbytes, *args, scratch=(), spec=VM):
    return pl.pallas_call(
        body,
        out_shape=outs,
        in_specs=[spec] * len(args),
        out_specs=jax.tree.map(lambda _: VM, outs),
        scratch_shapes=scratch,
        compiler_params=pltpu.CompilerParams(vmem_limit_bytes=GRANT),
        cost_estimate=pl.CostEstimate(flops=flops, bytes_accessed=nbytes, transcendentals=0),
    )(*args)


def shape(dims, dtype):
    return jax.ShapeDtypeStruct(dims, dtype)


def in_vmem(array):
    return pltpu.with_memory_space_constraint(array, pltpu.VMEM)


def in_hbm(array):
    return pltpu.with_memory_space_constraint(array, pltpu.HBM)


def slots(ids_t, columns):
    count = ids_t.shape[1]
    held = jnp.max(jnp.where(ids_t == 0, 1.0, 0.0), axis=0, keepdims=True)
    row = lax.broadcasted_iota(jnp.int32, (count, count), 0)
    col = lax.broadcasted_iota(jnp.int32, (count, count), 1)
    spread = jnp.broadcast_to(held, (count, count))
    rank = jnp.sum(jnp.where(col < row, spread, 0.0), axis=1, keepdims=True)
    routed = jnp.sum(jnp.where(col == row, spread, 0.0), axis=1, keepdims=True)
    slot = (lax.broadcasted_iota(jnp.int32, (count, columns), 1) % MOST).astype(F32)
    return jnp.where((slot == rank) & (routed > 0.0), 1.0, 0.0).astype(BF16)


def pack_body(ids_hbm, tokens_hbm, out_ref, ids_ref, tokens_ref, sems):
    copies = [
        pltpu.make_async_copy(ids_hbm, ids_ref, sems.at[0]),
        pltpu.make_async_copy(tokens_hbm, tokens_ref, sems.at[1]),
    ]
    for copy in copies:
        copy.start()
    copies[0].wait()
    one_hot = slots(ids_ref[...], MOST)
    copies[1].wait()
    out_ref[...] = lax.dot_general(
        one_hot, tokens_ref[...], (((0,), (0,)), ((), ())), preferred_element_type=F32
    ).astype(BF16)


def bit_order(spot):
    return (spot % 2) * 2 + spot // 2


def gather_body(*refs):
    out_ref = refs[-1]
    place = (lax.axis_index("dp") % 2) ^ lax.axis_index("tp")
    for q, block in enumerate(refs[:-1]):
        spot = bit_order(place ^ q)
        out_ref[pl.ds(pl.multiple_of(spot * MOST, MOST), MOST), :] = block[...]


def gate_up(rows, weights, keep_ref, send_ref, low, high):
    half = rows.shape[0] // 2
    for k, weight in enumerate(weights):
        for at in range(low, high, WIDE):
            to = min(at + WIDE, high)
            part = jnp.dot(rows, weight[:, at:to], preferred_element_type=F32).astype(BF16)
            keep_ref[k, :, at - low : to - low] = part[:half]
            send_ref[k, :, at - low : to - low] = part[half:]


def first_body(low, high, *refs):
    blocks = refs[:-5]
    gate_ref, up_ref, keep_ref, send_ref, rows_ref = refs[-5:]
    gather_body(*blocks, rows_ref)
    gate_up(rows_ref[...], (gate_ref, up_ref), keep_ref, send_ref, low, high)


def later_body(low, high, rows_ref, gate_ref, up_ref, keep_ref, send_ref):
    gate_up(rows_ref[...], (gate_ref, up_ref), keep_ref, send_ref, low, high)


def fold_body(keep_ref, got_ref, own_ref, send_ref):
    total = keep_ref[...].astype(F32) + got_ref[...].astype(F32)
    own_ref[...] = total
    send_ref[...] = total.astype(BF16)


def hidden_body(own_ref, got_ref, out_ref):
    total = own_ref[...] + got_ref[...].astype(F32)
    gate, up = total[0], total[1]
    out_ref[...] = (gate / (1.0 + jnp.exp(-gate)) * up).astype(BF16)


def down_body(low, high, mine_ref, beside_ref, weight_ref, *refs):
    hidden = jnp.concatenate([mine_ref[...], beside_ref[...]], axis=0)
    value = jnp.dot(hidden, weight_ref[low:high, :], preferred_element_type=F32)
    refs[-1][...] = value + refs[0][...] if len(refs) > 1 else value


def last_body(n_tp, low, high, mine_ref, beside_ref, weight_ref, total_ref, own_ref, *refs):
    sends, scratch = refs[:-1], refs[-1]
    down_body(low, high, mine_ref, beside_ref, weight_ref, total_ref, scratch)
    place = (lax.axis_index("dp") % 2) ^ lax.axis_index("tp")
    for q in range(n_tp):
        block = scratch[pl.ds(pl.multiple_of(bit_order(place ^ q) * MOST, MOST), MOST), :]
        if q == 0:
            own_ref[...] = block
        else:
            sends[q - 1][...] = block.astype(BF16)


def final_body(ids_ref, route_ref, own_ref, *refs):
    out_ref = refs[-1]
    own = own_ref[...]
    high = own.astype(BF16)
    rest = own - high.astype(F32)
    mid = rest.astype(BF16)
    low = (rest - mid.astype(F32)).astype(BF16)
    terms = jnp.concatenate([high, mid, low] + [got[...] for got in refs[:-1]], axis=0)
    ids = ids_ref[...]
    count = ids.shape[1]
    held = jnp.sum(jnp.where(ids == 0, route_ref[...], 0.0), axis=0, keepdims=True)
    row = lax.broadcasted_iota(jnp.int32, (count, count), 0)
    col = lax.broadcasted_iota(jnp.int32, (count, count), 1)
    combine = jnp.sum(
        jnp.where(col == row, jnp.broadcast_to(held, (count, count)), 0.0), axis=1, keepdims=True
    )
    spread = jnp.dot(slots(ids, terms.shape[0]), terms, preferred_element_type=F32)
    out_ref[...] = (combine * spread).astype(BF16)


def swap(value, axis, size, mask):
    return lax.ppermute(value, axis, [(i, i ^ mask) for i in range(size)])


def direct(n_dp, n_tp, tokens, gate_weight, up_weight, down_weight, expert_ids, route_weights):
    ids_t, route_t = expert_ids.T, route_weights.T
    model, width = gate_weight.shape
    out_width = down_weight.shape[1]
    total = MOST * n_tp
    gate_weight, up_weight, down_weight = map(in_vmem, (gate_weight, up_weight, down_weight))
    packed = call(
        pack_body,
        shape((MOST, model), BF16),
        PRIOR * total * model * width,
        PRIOR * model * width,
        in_hbm(ids_t),
        in_hbm(tokens),
        scratch=[
            pltpu.VMEM(ids_t.shape, ids_t.dtype),
            pltpu.VMEM(tokens.shape, tokens.dtype),
            pltpu.SemaphoreType.DMA((2,)),
        ],
        spec=pl.BlockSpec(memory_space=pltpu.HBM),
    )
    blocks = [packed]
    for q in range(1, n_tp):
        blocks.append(swap(packed, "tp", n_tp, q))
    cuts = [width * cut // 16 for cut in CUTS]
    spans = list(zip(cuts[:-1], cuts[1:]))
    folded = []
    for c, (low, high) in enumerate(spans):
        dims = (2, total // 2, high - low)
        cost = 4 * total * model * (high - low), 4 * model * (high - low)
        if c == 0:
            keep, send, rows = call(
                functools.partial(first_body, low, high),
                [shape(dims, BF16)] * 2 + [shape((total, model), BF16)],
                *cost,
                *blocks,
                gate_weight,
                up_weight,
            )
        else:
            keep, send = call(
                functools.partial(later_body, low, high),
                [shape(dims, BF16)] * 2,
                *cost,
                rows,
                gate_weight,
                up_weight,
            )
        got = swap(send, "dp", n_dp, 1)
        folded.append(
            call(fold_body, [shape(dims, F32), shape(dims, BF16)], total * width, 6 * total * width, keep, got)
        )
    value = []
    for c, (low, high) in enumerate(spans):
        own, send = folded[c]
        got = swap(send, "dp", n_dp, 2)
        mine = call(
            hidden_body, shape(own.shape[1:], BF16), total * width, 3 * total * width, own, got
        )
        beside = swap(mine, "dp", n_dp, 1)
        cost = 2 * total * (high - low) * out_width, 2 * (high - low) * out_width
        last = c == len(spans) - 1
        value = call(
            functools.partial(last_body, n_tp, low, high) if last else functools.partial(down_body, low, high),
            [shape((MOST, out_width), F32)] + [shape((MOST, out_width), BF16)] * (n_tp - 1)
            if last
            else [shape((total, out_width), F32)],
            *cost,
            mine,
            beside,
            down_weight,
            *value,
            scratch=[pltpu.VMEM((total, out_width), F32)] if last else (),
        )
    own, *sends = value
    got = []
    for q, send in enumerate(sends):
        got.append(swap(send, "tp", n_tp, q + 1))
    return call(
        final_body, shape((tokens.shape[0], out_width), BF16), 2 * tokens.size, 4 * tokens.size,
        ids_t, route_t, own, *got,
    )


def general(tokens, gate_weight, up_weight, down_weight, expert_ids, route_weights):
    held_mask = expert_ids == 0
    combine = jnp.sum(jnp.where(held_mask, route_weights, jnp.zeros_like(route_weights)), axis=1)
    hidden_width = gate_weight.shape[1]
    routed = jnp.any(held_mask, axis=1)
    slot_rank = jnp.cumsum(routed.astype(jnp.int32)) - 1
    slot_ids = jnp.arange(MOST, dtype=jnp.int32)
    dispatch = ((slot_rank[None, :] == slot_ids[:, None]) & routed[None, :]).astype(BF16)
    packed = jnp.dot(dispatch, tokens, preferred_element_type=F32).astype(BF16)
    row_block = lax.all_gather(packed, "tp", axis=0, tiled=True)
    gate_part = jnp.dot(row_block, gate_weight, preferred_element_type=F32).astype(BF16)
    up_part = jnp.dot(row_block, up_weight, preferred_element_type=F32).astype(BF16)
    gate_up = jnp.concatenate([gate_part, up_part], axis=1)
    summed = lax.psum(gate_up, "dp").astype(F32)
    hidden = (jax.nn.silu(summed[:, :hidden_width]) * summed[:, hidden_width:]).astype(BF16)
    partial_value = jnp.dot(hidden, down_weight, preferred_element_type=F32)
    result = jnp.dot(
        dispatch.T.astype(F32),
        lax.psum_scatter(
            partial_value.astype(BF16), "tp", scatter_dimension=0, tiled=True
        ).astype(F32),
        precision=lax.Precision.HIGHEST,
    )
    return (combine[:, None] * result).astype(BF16)


def solution(mesh):
    n_dp, n_tp = mesh.shape["dp"], mesh.shape["tp"]
    in_specs = (
        P(("groups", "tp"), "dp"),
        P("dp", "tp"),
        P("dp", "tp"),
        P("tp", "dp"),
        P(("groups", "tp"), None),
        P(("groups", "tp"), None),
    )
    out_specs = P(("groups", "tp"), "dp")
    def specialised(*args):
        return direct(n_dp, n_tp, *args)

    fits = n_dp == n_tp == 4
    return jax.shard_map(
        specialised if fits else general,
        mesh=mesh,
        in_specs=in_specs,
        out_specs=out_specs,
        check_vma=False,
    )
```

```python
import functools

import jax
import jax.numpy as jnp
from jax import lax
from jax.experimental import pallas as pl
from jax.experimental.pallas import tpu as pltpu
from jax.sharding import PartitionSpec as P


MOST = 16
F32 = jnp.float32
BF16 = jnp.bfloat16
PRIOR = 100000
WIDE = 2048
PIECES = 2
CUTS = (0, 4, 8, 12, 16)
GRANT = 2 * 1024 * 1024
VM = pl.BlockSpec(memory_space=pltpu.VMEM)


def call(body, outs, flops, nbytes, *args, scratch=(), spec=VM, out_spec=VM):
    return pl.pallas_call(
        body,
        out_shape=outs,
        in_specs=[spec] * len(args),
        out_specs=jax.tree.map(lambda _: out_spec, outs),
        scratch_shapes=scratch,
        compiler_params=pltpu.CompilerParams(vmem_limit_bytes=GRANT),
        cost_estimate=pl.CostEstimate(flops=flops, bytes_accessed=nbytes, transcendentals=0),
    )(*args)


def shape(dims, dtype):
    return jax.ShapeDtypeStruct(dims, dtype)


def in_vmem(array):
    return pltpu.with_memory_space_constraint(array, pltpu.VMEM)


def in_hbm(array):
    return pltpu.with_memory_space_constraint(array, pltpu.HBM)


def slots(ids_t, columns):
    count = ids_t.shape[1]
    held = jnp.max(jnp.where(ids_t == 0, 1.0, 0.0), axis=0, keepdims=True)
    row = lax.broadcasted_iota(jnp.int32, (count, count), 0)
    col = lax.broadcasted_iota(jnp.int32, (count, count), 1)
    spread = jnp.broadcast_to(held, (count, count))
    rank = jnp.sum(jnp.where(col < row, spread, 0.0), axis=1, keepdims=True)
    routed = jnp.sum(jnp.where(col == row, spread, 0.0), axis=1, keepdims=True)
    slot = (lax.broadcasted_iota(jnp.int32, (count, columns), 1) % MOST).astype(F32)
    return jnp.where((slot == rank) & (routed > 0.0), 1.0, 0.0).astype(BF16)


def pack_body(ids_hbm, routes_hbm, tokens_hbm, out_ref, slots_ref, combine_ref, ids_ref, routes_ref, tokens_ref, sems):
    copies = [
        pltpu.make_async_copy(source, target, sems.at[i])
        for i, (source, target) in enumerate(
            ((tokens_hbm, tokens_ref), (ids_hbm, ids_ref), (routes_hbm, routes_ref))
        )
    ]
    for copy in copies:
        copy.start()
    copies[1].wait()
    copies[2].wait()
    ids = ids_ref[...]
    count = ids.shape[1]
    slots_ref[...] = slots(ids, slots_ref.shape[1])
    held = jnp.sum(jnp.where(ids == 0, routes_ref[...], 0.0), axis=0, keepdims=True)
    row = lax.broadcasted_iota(jnp.int32, (count, count), 0)
    col = lax.broadcasted_iota(jnp.int32, (count, count), 1)
    combine_ref[...] = jnp.sum(
        jnp.where(col == row, jnp.broadcast_to(held, (count, count)), 0.0), axis=1, keepdims=True
    )
    one_hot = slots(ids, MOST)
    copies[0].wait()
    out_ref[...] = lax.dot_general(
        one_hot, tokens_ref[...], (((0,), (0,)), ((), ())), preferred_element_type=F32
    ).astype(BF16)


def bit_order(spot):
    return (spot % 2) * 2 + spot // 2


def gather_body(*refs):
    out_ref = refs[-1]
    place = (lax.axis_index("dp") % 2) ^ lax.axis_index("tp")
    for q, block in enumerate(refs[:-1]):
        spot = bit_order(place ^ q)
        out_ref[pl.ds(pl.multiple_of(spot * MOST, MOST), MOST), :] = block[...]


def gate_up(rows, weights, keep_ref, send_ref, low, high):
    half = rows.shape[0] // 2
    for k, weight in enumerate(weights):
        for at in range(low, high, WIDE):
            to = min(at + WIDE, high)
            part = jnp.dot(rows, weight[:, at:to], preferred_element_type=F32).astype(BF16)
            keep_ref[k, :, at - low : to - low] = part[:half]
            send_ref[k, :, at - low : to - low] = part[half:]


def first_body(low, high, *refs):
    blocks = refs[:-5]
    gate_ref, up_ref, keep_ref, send_ref, rows_ref = refs[-5:]
    gather_body(*blocks, rows_ref)
    gate_up(rows_ref[...], (gate_ref, up_ref), keep_ref, send_ref, low, high)


def later_body(low, high, rows_ref, gate_ref, up_ref, keep_ref, send_ref):
    gate_up(rows_ref[...], (gate_ref, up_ref), keep_ref, send_ref, low, high)


def fold_body(keep_ref, got_ref, own_ref, send_ref):
    total = keep_ref[...].astype(F32) + got_ref[...].astype(F32)
    own_ref[...] = total
    send_ref[...] = total.astype(BF16)


def hidden_body(own_ref, got_ref, out_ref):
    total = own_ref[...] + got_ref[...].astype(F32)
    gate, up = total[0], total[1]
    out_ref[...] = (gate / (1.0 + jnp.exp(-gate)) * up).astype(BF16)


def down_body(low, high, mine_ref, beside_ref, weight_ref, *refs):
    hidden = jnp.concatenate([mine_ref[...], beside_ref[...]], axis=0)
    value = jnp.dot(hidden, weight_ref[low:high, :], preferred_element_type=F32)
    refs[-1][...] = value + refs[0][...] if len(refs) > 1 else value


def last_body(n_tp, low, high, mine_ref, beside_ref, weight_ref, total_ref, own_ref, *refs):
    sends, scratch = refs[:-1], refs[-1]
    down_body(low, high, mine_ref, beside_ref, weight_ref, total_ref, scratch)
    place = (lax.axis_index("dp") % 2) ^ lax.axis_index("tp")
    for q in range(n_tp):
        block = scratch[pl.ds(pl.multiple_of(bit_order(place ^ q) * MOST, MOST), MOST), :]
        if q == 0:
            own_ref[...] = block
        else:
            sends[q - 1][...] = block.astype(BF16)


def final_body(slots_ref, combine_ref, own_ref, *refs):
    *gots, out_hbm, out_ref, sems = refs
    width = out_ref.shape[1] // PIECES
    copies = []
    for i in range(PIECES):
        at = slice(i * width, (i + 1) * width)
        own = own_ref[:, at]
        high = own.astype(BF16)
        rest = own - high.astype(F32)
        mid = rest.astype(BF16)
        low = (rest - mid.astype(F32)).astype(BF16)
        terms = jnp.concatenate([high, mid, low] + [got[:, at] for got in gots], axis=0)
        spread = jnp.dot(slots_ref[...], terms, preferred_element_type=F32)
        out_ref[:, at] = (combine_ref[...] * spread).astype(BF16)
        copies.append(pltpu.make_async_copy(out_ref.at[:, at], out_hbm.at[:, at], sems.at[i]))
        copies[i].start()
    for copy in copies:
        copy.wait()


def swap(value, axis, size, mask):
    return lax.ppermute(value, axis, [(i, i ^ mask) for i in range(size)])


def direct(n_dp, n_tp, tokens, gate_weight, up_weight, down_weight, expert_ids, route_weights):
    ids_t, route_t = expert_ids.T, route_weights.T
    model, width = gate_weight.shape
    out_width = down_weight.shape[1]
    total = MOST * n_tp
    gate_weight, up_weight, down_weight = map(in_vmem, (gate_weight, up_weight, down_weight))
    count = tokens.shape[0]
    packed, spot, combine = call(
        pack_body,
        [shape((MOST, model), BF16), shape((count, (n_tp + 2) * MOST), BF16), shape((count, 1), F32)],
        PRIOR * total * model * width,
        PRIOR * model * width,
        in_hbm(ids_t),
        in_hbm(route_t),
        in_hbm(tokens),
        scratch=[
            pltpu.VMEM(ids_t.shape, ids_t.dtype),
            pltpu.VMEM(route_t.shape, route_t.dtype),
            pltpu.VMEM(tokens.shape, tokens.dtype),
            pltpu.SemaphoreType.DMA((3,)),
        ],
        spec=pl.BlockSpec(memory_space=pltpu.HBM),
    )
    blocks = [packed]
    for q in range(1, n_tp):
        blocks.append(swap(packed, "tp", n_tp, q))
    cuts = [width * cut // 16 for cut in CUTS]
    spans = list(zip(cuts[:-1], cuts[1:]))
    folded = []
    for c, (low, high) in enumerate(spans):
        dims = (2, total // 2, high - low)
        cost = 4 * total * model * (high - low), 4 * model * (high - low)
        if c == 0:
            keep, send, rows = call(
                functools.partial(first_body, low, high),
                [shape(dims, BF16)] * 2 + [shape((total, model), BF16)],
                *cost,
                *blocks,
                gate_weight,
                up_weight,
            )
        else:
            keep, send = call(
                functools.partial(later_body, low, high),
                [shape(dims, BF16)] * 2,
                *cost,
                rows,
                gate_weight,
                up_weight,
            )
        got = swap(send, "dp", n_dp, 1)
        folded.append(
            call(fold_body, [shape(dims, F32), shape(dims, BF16)], total * width, 6 * total * width, keep, got)
        )
    value = []
    for c, (low, high) in enumerate(spans):
        own, send = folded[c]
        got = swap(send, "dp", n_dp, 2)
        mine = call(
            hidden_body, shape(own.shape[1:], BF16), total * width, 3 * total * width, own, got
        )
        beside = swap(mine, "dp", n_dp, 1)
        cost = 2 * total * (high - low) * out_width, 2 * (high - low) * out_width
        last = c == len(spans) - 1
        value = call(
            functools.partial(last_body, n_tp, low, high) if last else functools.partial(down_body, low, high),
            [shape((MOST, out_width), F32)] + [shape((MOST, out_width), BF16)] * (n_tp - 1)
            if last
            else [shape((total, out_width), F32)],
            *cost,
            mine,
            beside,
            down_weight,
            *value,
            scratch=[pltpu.VMEM((total, out_width), F32)] if last else (),
        )
    own, *sends = value
    got = []
    for q, send in enumerate(sends):
        got.append(swap(send, "tp", n_tp, q + 1))
    dims = (count, out_width)
    return call(
        final_body,
        shape(dims, BF16),
        2 * tokens.size,
        4 * tokens.size,
        spot,
        combine,
        own,
        *got,
        scratch=[pltpu.VMEM(dims, BF16), pltpu.SemaphoreType.DMA((PIECES,))],
        out_spec=pl.BlockSpec(memory_space=pltpu.HBM),
    )


def general(tokens, gate_weight, up_weight, down_weight, expert_ids, route_weights):
    held_mask = expert_ids == 0
    combine = jnp.sum(jnp.where(held_mask, route_weights, jnp.zeros_like(route_weights)), axis=1)
    hidden_width = gate_weight.shape[1]
    routed = jnp.any(held_mask, axis=1)
    slot_rank = jnp.cumsum(routed.astype(jnp.int32)) - 1
    slot_ids = jnp.arange(MOST, dtype=jnp.int32)
    dispatch = ((slot_rank[None, :] == slot_ids[:, None]) & routed[None, :]).astype(BF16)
    packed = jnp.dot(dispatch, tokens, preferred_element_type=F32).astype(BF16)
    row_block = lax.all_gather(packed, "tp", axis=0, tiled=True)
    gate_part = jnp.dot(row_block, gate_weight, preferred_element_type=F32).astype(BF16)
    up_part = jnp.dot(row_block, up_weight, preferred_element_type=F32).astype(BF16)
    gate_up = jnp.concatenate([gate_part, up_part], axis=1)
    summed = lax.psum(gate_up, "dp").astype(F32)
    hidden = (jax.nn.silu(summed[:, :hidden_width]) * summed[:, hidden_width:]).astype(BF16)
    partial_value = jnp.dot(hidden, down_weight, preferred_element_type=F32)
    result = jnp.dot(
        dispatch.T.astype(F32),
        lax.psum_scatter(
            partial_value.astype(BF16), "tp", scatter_dimension=0, tiled=True
        ).astype(F32),
        precision=lax.Precision.HIGHEST,
    )
    return (combine[:, None] * result).astype(BF16)


def solution(mesh):
    n_dp, n_tp = mesh.shape["dp"], mesh.shape["tp"]
    in_specs = (
        P(("groups", "tp"), "dp"),
        P("dp", "tp"),
        P("dp", "tp"),
        P("tp", "dp"),
        P(("groups", "tp"), None),
        P(("groups", "tp"), None),
    )
    out_specs = P(("groups", "tp"), "dp")
    def specialised(*args):
        return direct(n_dp, n_tp, *args)

    fits = n_dp == n_tp == 4
    return jax.shard_map(
        specialised if fits else general,
        mesh=mesh,
        in_specs=in_specs,
        out_specs=out_specs,
        check_vma=False,
    )
```

```python
import functools

import jax
import jax.numpy as jnp
from jax import lax
from jax.experimental import pallas as pl
from jax.experimental.pallas import tpu as pltpu
from jax.sharding import PartitionSpec as P


MOST = 16
F32 = jnp.float32
BF16 = jnp.bfloat16
PRIOR = 100000
WIDE = 2048
PIECES = 2
CUTS = (0, 4, 8, 12, 16)
GRANT = 2 * 1024 * 1024
VM = pl.BlockSpec(memory_space=pltpu.VMEM)


def call(body, outs, flops, nbytes, *args, scratch=(), spec=VM, out_spec=VM):
    return pl.pallas_call(
        body,
        out_shape=outs,
        in_specs=[spec] * len(args),
        out_specs=jax.tree.map(lambda _: out_spec, outs),
        scratch_shapes=scratch,
        compiler_params=pltpu.CompilerParams(vmem_limit_bytes=GRANT),
        cost_estimate=pl.CostEstimate(flops=flops, bytes_accessed=nbytes, transcendentals=0),
    )(*args)


def shape(dims, dtype):
    return jax.ShapeDtypeStruct(dims, dtype)


def in_vmem(array):
    return pltpu.with_memory_space_constraint(array, pltpu.VMEM)


def in_hbm(array):
    return pltpu.with_memory_space_constraint(array, pltpu.HBM)


def slots(ids_t, columns):
    count = ids_t.shape[1]
    held = jnp.max(jnp.where(ids_t == 0, 1.0, 0.0), axis=0, keepdims=True)
    row = lax.broadcasted_iota(jnp.int32, (count, count), 0)
    col = lax.broadcasted_iota(jnp.int32, (count, count), 1)
    spread = jnp.broadcast_to(held, (count, count))
    rank = jnp.sum(jnp.where(col < row, spread, 0.0), axis=1, keepdims=True)
    routed = jnp.sum(jnp.where(col == row, spread, 0.0), axis=1, keepdims=True)
    slot = (lax.broadcasted_iota(jnp.int32, (count, columns), 1) % MOST).astype(F32)
    return jnp.where((slot == rank) & (routed > 0.0), 1.0, 0.0).astype(BF16)


def pack_body(ids_hbm, routes_hbm, tokens_hbm, out_ref, slots_ref, combine_ref, ids_ref, routes_ref, tokens_ref, sems):
    copies = [
        pltpu.make_async_copy(source, target, sems.at[i])
        for i, (source, target) in enumerate(
            ((tokens_hbm, tokens_ref), (ids_hbm, ids_ref), (routes_hbm, routes_ref))
        )
    ]
    for copy in copies:
        copy.start()
    copies[1].wait()
    copies[2].wait()
    ids = ids_ref[...]
    count = ids.shape[1]
    slots_ref[...] = slots(ids, slots_ref.shape[1])
    held = jnp.sum(jnp.where(ids == 0, routes_ref[...], 0.0), axis=0, keepdims=True)
    row = lax.broadcasted_iota(jnp.int32, (count, count), 0)
    col = lax.broadcasted_iota(jnp.int32, (count, count), 1)
    combine_ref[...] = jnp.sum(
        jnp.where(col == row, jnp.broadcast_to(held, (count, count)), 0.0), axis=1, keepdims=True
    )
    one_hot = slots(ids, MOST)
    copies[0].wait()
    out_ref[...] = lax.dot_general(
        one_hot, tokens_ref[...], (((0,), (0,)), ((), ())), preferred_element_type=F32
    ).astype(BF16)


def bit_order(spot, count):
    return (spot % 2) * (count // 2) + spot // 2


def gather_body(*refs):
    out_ref = refs[-1]
    place = (lax.axis_index("dp") % 2) ^ lax.axis_index("tp")
    for q, block in enumerate(refs[:-1]):
        spot = bit_order(place ^ q, len(refs) - 1)
        out_ref[pl.ds(pl.multiple_of(spot * MOST, MOST), MOST), :] = block[...]


def gate_up(rows, weights, keep_ref, send_ref, low, high):
    half = rows.shape[0] // 2
    for k, weight in enumerate(weights):
        for at in range(low, high, WIDE):
            to = min(at + WIDE, high)
            part = jnp.dot(rows, weight[:, at:to], preferred_element_type=F32).astype(BF16)
            keep_ref[k, :, at - low : to - low] = part[:half]
            send_ref[k, :, at - low : to - low] = part[half:]


def first_body(low, high, *refs):
    blocks = refs[:-5]
    gate_ref, up_ref, keep_ref, send_ref, rows_ref = refs[-5:]
    gather_body(*blocks, rows_ref)
    gate_up(rows_ref[...], (gate_ref, up_ref), keep_ref, send_ref, low, high)


def later_body(low, high, rows_ref, gate_ref, up_ref, keep_ref, send_ref):
    gate_up(rows_ref[...], (gate_ref, up_ref), keep_ref, send_ref, low, high)


def fold_body(keep_ref, got_ref, own_ref, send_ref):
    total = keep_ref[...].astype(F32) + got_ref[...].astype(F32)
    own_ref[...] = total
    send_ref[...] = total.astype(BF16)


def hidden_body(own_ref, got_ref, out_ref):
    total = own_ref[...] + got_ref[...].astype(F32)
    gate, up = total[0], total[1]
    out_ref[...] = (gate / (1.0 + jnp.exp(-gate)) * up).astype(BF16)


def down_body(low, high, mine_ref, beside_ref, weight_ref, *refs):
    hidden = jnp.concatenate([mine_ref[...], beside_ref[...]], axis=0)
    value = jnp.dot(hidden, weight_ref[low:high, :], preferred_element_type=F32)
    refs[-1][...] = value + refs[0][...] if len(refs) > 1 else value


def last_body(n_tp, low, high, mine_ref, beside_ref, weight_ref, total_ref, own_ref, *refs):
    sends, scratch = refs[:-1], refs[-1]
    down_body(low, high, mine_ref, beside_ref, weight_ref, total_ref, scratch)
    place = (lax.axis_index("dp") % 2) ^ lax.axis_index("tp")
    for q in range(n_tp):
        block = scratch[pl.ds(pl.multiple_of(bit_order(place ^ q, n_tp) * MOST, MOST), MOST), :]
        if q == 0:
            own_ref[...] = block
        else:
            sends[q - 1][...] = block.astype(BF16)


def final_body(slots_ref, combine_ref, own_ref, *refs):
    *gots, out_hbm, out_ref, sems = refs
    width = out_ref.shape[1] // PIECES
    copies = []
    for i in range(PIECES):
        at = slice(i * width, (i + 1) * width)
        own = own_ref[:, at]
        high = own.astype(BF16)
        rest = own - high.astype(F32)
        mid = rest.astype(BF16)
        low = (rest - mid.astype(F32)).astype(BF16)
        terms = jnp.concatenate([high, mid, low] + [got[:, at] for got in gots], axis=0)
        spread = jnp.dot(slots_ref[...], terms, preferred_element_type=F32)
        out_ref[:, at] = (combine_ref[...] * spread).astype(BF16)
        copies.append(pltpu.make_async_copy(out_ref.at[:, at], out_hbm.at[:, at], sems.at[i]))
        copies[i].start()
    for copy in copies:
        copy.wait()


def swap(value, axis, size, mask):
    return lax.ppermute(value, axis, [(i, i ^ mask) for i in range(size)])


def direct(n_dp, n_tp, tokens, gate_weight, up_weight, down_weight, expert_ids, route_weights):
    ids_t, route_t = expert_ids.T, route_weights.T
    model, width = gate_weight.shape
    out_width = down_weight.shape[1]
    total = MOST * n_tp
    gate_weight, up_weight, down_weight = map(in_vmem, (gate_weight, up_weight, down_weight))
    count = tokens.shape[0]
    packed, spot, combine = call(
        pack_body,
        [shape((MOST, model), BF16), shape((count, (n_tp + 2) * MOST), BF16), shape((count, 1), F32)],
        PRIOR * total * model * width,
        PRIOR * model * width,
        in_hbm(ids_t),
        in_hbm(route_t),
        in_hbm(tokens),
        scratch=[
            pltpu.VMEM(ids_t.shape, ids_t.dtype),
            pltpu.VMEM(route_t.shape, route_t.dtype),
            pltpu.VMEM(tokens.shape, tokens.dtype),
            pltpu.SemaphoreType.DMA((3,)),
        ],
        spec=pl.BlockSpec(memory_space=pltpu.HBM),
    )
    blocks = [packed]
    for q in range(1, n_tp):
        blocks.append(swap(packed, "tp", n_tp, q))
    cuts = [width * cut // 16 for cut in CUTS]
    spans = list(zip(cuts[:-1], cuts[1:]))
    folded = []
    for c, (low, high) in enumerate(spans):
        dims = (2, total // 2, high - low)
        cost = 4 * total * model * (high - low), 4 * model * (high - low)
        if c == 0:
            keep, send, rows = call(
                functools.partial(first_body, low, high),
                [shape(dims, BF16)] * 2 + [shape((total, model), BF16)],
                *cost,
                *blocks,
                gate_weight,
                up_weight,
            )
        else:
            keep, send = call(
                functools.partial(later_body, low, high),
                [shape(dims, BF16)] * 2,
                *cost,
                rows,
                gate_weight,
                up_weight,
            )
        got = swap(send, "dp", n_dp, 1)
        folded.append(
            call(fold_body, [shape(dims, F32), shape(dims, BF16)], total * width, 6 * total * width, keep, got)
        )
    value = []
    for c, (low, high) in enumerate(spans):
        own, send = folded[c]
        got = swap(send, "dp", n_dp, 2)
        mine = call(
            hidden_body, shape(own.shape[1:], BF16), total * width, 3 * total * width, own, got
        )
        beside = swap(mine, "dp", n_dp, 1)
        cost = 2 * total * (high - low) * out_width, 2 * (high - low) * out_width
        last = c == len(spans) - 1
        value = call(
            functools.partial(last_body, n_tp, low, high) if last else functools.partial(down_body, low, high),
            [shape((MOST, out_width), F32)] + [shape((MOST, out_width), BF16)] * (n_tp - 1)
            if last
            else [shape((total, out_width), F32)],
            *cost,
            mine,
            beside,
            down_weight,
            *value,
            scratch=[pltpu.VMEM((total, out_width), F32)] if last else (),
        )
    own, *sends = value
    got = []
    for q, send in enumerate(sends):
        got.append(swap(send, "tp", n_tp, q + 1))
    dims = (count, out_width)
    return call(
        final_body,
        shape(dims, BF16),
        2 * tokens.size,
        4 * tokens.size,
        spot,
        combine,
        own,
        *got,
        scratch=[pltpu.VMEM(dims, BF16), pltpu.SemaphoreType.DMA((PIECES,))],
        out_spec=pl.BlockSpec(memory_space=pltpu.HBM),
    )


def general(tokens, gate_weight, up_weight, down_weight, expert_ids, route_weights):
    held_mask = expert_ids == 0
    combine = jnp.sum(jnp.where(held_mask, route_weights, jnp.zeros_like(route_weights)), axis=1)
    hidden_width = gate_weight.shape[1]
    routed = jnp.any(held_mask, axis=1)
    slot_rank = jnp.cumsum(routed.astype(jnp.int32)) - 1
    slot_ids = jnp.arange(MOST, dtype=jnp.int32)
    dispatch = ((slot_rank[None, :] == slot_ids[:, None]) & routed[None, :]).astype(BF16)
    packed = jnp.dot(dispatch, tokens, preferred_element_type=F32).astype(BF16)
    row_block = lax.all_gather(packed, "tp", axis=0, tiled=True)
    gate_part = jnp.dot(row_block, gate_weight, preferred_element_type=F32).astype(BF16)
    up_part = jnp.dot(row_block, up_weight, preferred_element_type=F32).astype(BF16)
    gate_up = jnp.concatenate([gate_part, up_part], axis=1)
    summed = lax.psum(gate_up, "dp").astype(F32)
    hidden = (jax.nn.silu(summed[:, :hidden_width]) * summed[:, hidden_width:]).astype(BF16)
    partial_value = jnp.dot(hidden, down_weight, preferred_element_type=F32)
    result = jnp.dot(
        dispatch.T.astype(F32),
        lax.psum_scatter(
            partial_value.astype(BF16), "tp", scatter_dimension=0, tiled=True
        ).astype(F32),
        precision=lax.Precision.HIGHEST,
    )
    return (combine[:, None] * result).astype(BF16)


def solution(mesh):
    n_dp, n_tp = mesh.shape["dp"], mesh.shape["tp"]
    in_specs = (
        P(("groups", "tp"), "dp"),
        P("dp", "tp"),
        P("dp", "tp"),
        P("tp", "dp"),
        P(("groups", "tp"), None),
        P(("groups", "tp"), None),
    )
    out_specs = P(("groups", "tp"), "dp")
    def specialised(*args):
        return direct(n_dp, n_tp, *args)

    fits = n_dp == 4 and n_tp in (2, 4, 8)
    return jax.shard_map(
        specialised if fits else general,
        mesh=mesh,
        in_specs=in_specs,
        out_specs=out_specs,
        check_vma=False,
    )
```

```python
import functools

import jax
import jax.numpy as jnp
from jax import lax
from jax.experimental import pallas as pl
from jax.experimental.pallas import tpu as pltpu
from jax.sharding import PartitionSpec as P


MOST = 16
F32 = jnp.float32
BF16 = jnp.bfloat16
PRIOR = 100000
WIDE = 2048
PIECES = 2
CUTS = (0, 4, 8, 12, 16)
GRANT = 2 * 1024 * 1024
VM = pl.BlockSpec(memory_space=pltpu.VMEM)


def call(body, outs, flops, nbytes, *args, scratch=(), spec=VM, out_spec=VM):
    return pl.pallas_call(
        body,
        out_shape=outs,
        in_specs=[spec] * len(args),
        out_specs=jax.tree.map(lambda _: out_spec, outs),
        scratch_shapes=scratch,
        compiler_params=pltpu.CompilerParams(vmem_limit_bytes=GRANT),
        cost_estimate=pl.CostEstimate(flops=flops, bytes_accessed=nbytes, transcendentals=0),
    )(*args)


def shape(dims, dtype):
    return jax.ShapeDtypeStruct(dims, dtype)


def in_vmem(array):
    return pltpu.with_memory_space_constraint(array, pltpu.VMEM)


def in_hbm(array):
    return pltpu.with_memory_space_constraint(array, pltpu.HBM)


def slots(ids_t, columns):
    count = ids_t.shape[1]
    held = jnp.max(jnp.where(ids_t == 0, 1.0, 0.0), axis=0, keepdims=True)
    row = lax.broadcasted_iota(jnp.int32, (count, count), 0)
    col = lax.broadcasted_iota(jnp.int32, (count, count), 1)
    spread = jnp.broadcast_to(held, (count, count))
    rank = jnp.sum(jnp.where(col < row, spread, 0.0), axis=1, keepdims=True)
    routed = jnp.sum(jnp.where(col == row, spread, 0.0), axis=1, keepdims=True)
    slot = (lax.broadcasted_iota(jnp.int32, (count, columns), 1) % MOST).astype(F32)
    return jnp.where((slot == rank) & (routed > 0.0), 1.0, 0.0).astype(BF16)


def pack_body(ids_hbm, routes_hbm, tokens_hbm, out_ref, slots_ref, combine_ref, ids_ref, routes_ref, tokens_ref, sems):
    copies = [
        pltpu.make_async_copy(source, target, sems.at[i])
        for i, (source, target) in enumerate(
            ((tokens_hbm, tokens_ref), (ids_hbm, ids_ref), (routes_hbm, routes_ref))
        )
    ]
    for copy in copies:
        copy.start()
    copies[1].wait()
    copies[2].wait()
    ids = ids_ref[...]
    count = ids.shape[1]
    slots_ref[...] = slots(ids, slots_ref.shape[1])
    held = jnp.sum(jnp.where(ids == 0, routes_ref[...], 0.0), axis=0, keepdims=True)
    row = lax.broadcasted_iota(jnp.int32, (count, count), 0)
    col = lax.broadcasted_iota(jnp.int32, (count, count), 1)
    combine_ref[...] = jnp.sum(
        jnp.where(col == row, jnp.broadcast_to(held, (count, count)), 0.0), axis=1, keepdims=True
    )
    one_hot = slots(ids, MOST)
    copies[0].wait()
    out_ref[...] = lax.dot_general(
        one_hot, tokens_ref[...], (((0,), (0,)), ((), ())), preferred_element_type=F32
    ).astype(BF16)


def bit_order(spot, count):
    return (spot % 2) * (count // 2) + spot // 2


def gather_body(*refs):
    out_ref = refs[-1]
    place = (lax.axis_index("dp") % 2) ^ lax.axis_index("tp")
    for q, block in enumerate(refs[:-1]):
        spot = bit_order(place ^ q, len(refs) - 1)
        out_ref[pl.ds(pl.multiple_of(spot * MOST, MOST), MOST), :] = block[...]


def gate_up(rows, weights, keep_ref, send_ref, low, high):
    half = rows.shape[0] // 2
    for k, weight in enumerate(weights):
        for at in range(low, high, WIDE):
            to = min(at + WIDE, high)
            part = jnp.dot(rows, weight[:, at:to], preferred_element_type=F32).astype(BF16)
            keep_ref[k, :, at - low : to - low] = part[:half]
            send_ref[k, :, at - low : to - low] = part[half:]


def first_body(low, high, *refs):
    blocks = refs[:-5]
    gate_ref, up_ref, keep_ref, send_ref, rows_ref = refs[-5:]
    gather_body(*blocks, rows_ref)
    gate_up(rows_ref[...], (gate_ref, up_ref), keep_ref, send_ref, low, high)


def later_body(low, high, rows_ref, gate_ref, up_ref, keep_ref, send_ref):
    gate_up(rows_ref[...], (gate_ref, up_ref), keep_ref, send_ref, low, high)


def fold_body(keep_ref, got_ref, send_ref):
    send_ref[...] = (keep_ref[...].astype(F32) + got_ref[...].astype(F32)).astype(BF16)


def hidden_body(keep_ref, pair_ref, cross_ref, out_ref):
    total = keep_ref[...].astype(F32) + pair_ref[...].astype(F32) + cross_ref[...].astype(F32)
    gate, up = total[0], total[1]
    out_ref[...] = (gate / (1.0 + jnp.exp(-gate)) * up).astype(BF16)


def down_body(low, high, mine_ref, beside_ref, weight_ref, *refs):
    hidden = jnp.concatenate([mine_ref[...], beside_ref[...]], axis=0)
    value = jnp.dot(hidden, weight_ref[low:high, :], preferred_element_type=F32)
    refs[-1][...] = value + refs[0][...] if len(refs) > 1 else value


def last_body(n_tp, low, high, mine_ref, beside_ref, weight_ref, total_ref, own_ref, *refs):
    sends, scratch = refs[:-1], refs[-1]
    down_body(low, high, mine_ref, beside_ref, weight_ref, total_ref, scratch)
    place = (lax.axis_index("dp") % 2) ^ lax.axis_index("tp")
    for q in range(n_tp):
        block = scratch[pl.ds(pl.multiple_of(bit_order(place ^ q, n_tp) * MOST, MOST), MOST), :]
        if q == 0:
            own_ref[...] = block
        else:
            sends[q - 1][...] = block.astype(BF16)


def final_body(slots_ref, combine_ref, own_ref, *refs):
    *gots, out_hbm, out_ref, sems = refs
    width = out_ref.shape[1] // PIECES
    copies = []
    for i in range(PIECES):
        at = slice(i * width, (i + 1) * width)
        own = own_ref[:, at]
        high = own.astype(BF16)
        rest = own - high.astype(F32)
        mid = rest.astype(BF16)
        low = (rest - mid.astype(F32)).astype(BF16)
        terms = jnp.concatenate([high, mid, low] + [got[:, at] for got in gots], axis=0)
        spread = jnp.dot(slots_ref[...], terms, preferred_element_type=F32)
        out_ref[:, at] = (combine_ref[...] * spread).astype(BF16)
        copies.append(pltpu.make_async_copy(out_ref.at[:, at], out_hbm.at[:, at], sems.at[i]))
        copies[i].start()
    for copy in copies:
        copy.wait()


def swap(value, axis, size, mask):
    return lax.ppermute(value, axis, [(i, i ^ mask) for i in range(size)])


def direct(n_dp, n_tp, tokens, gate_weight, up_weight, down_weight, expert_ids, route_weights):
    ids_t, route_t = expert_ids.T, route_weights.T
    model, width = gate_weight.shape
    out_width = down_weight.shape[1]
    total = MOST * n_tp
    gate_weight, up_weight, down_weight = map(in_vmem, (gate_weight, up_weight, down_weight))
    count = tokens.shape[0]
    packed, spot, combine = call(
        pack_body,
        [shape((MOST, model), BF16), shape((count, (n_tp + 2) * MOST), BF16), shape((count, 1), F32)],
        PRIOR * total * model * width,
        PRIOR * model * width,
        in_hbm(ids_t),
        in_hbm(route_t),
        in_hbm(tokens),
        scratch=[
            pltpu.VMEM(ids_t.shape, ids_t.dtype),
            pltpu.VMEM(route_t.shape, route_t.dtype),
            pltpu.VMEM(tokens.shape, tokens.dtype),
            pltpu.SemaphoreType.DMA((3,)),
        ],
        spec=pl.BlockSpec(memory_space=pltpu.HBM),
    )
    blocks = [packed]
    for q in range(1, n_tp):
        blocks.append(swap(packed, "tp", n_tp, q))
    cuts = [width * cut // 16 for cut in CUTS]
    spans = list(zip(cuts[:-1], cuts[1:]))
    folded = []
    for c, (low, high) in enumerate(spans):
        dims = (2, total // 2, high - low)
        cost = 4 * total * model * (high - low), 4 * model * (high - low)
        if c == 0:
            keep, send, rows = call(
                functools.partial(first_body, low, high),
                [shape(dims, BF16)] * 2 + [shape((total, model), BF16)],
                *cost,
                *blocks,
                gate_weight,
                up_weight,
            )
        else:
            keep, send = call(
                functools.partial(later_body, low, high),
                [shape(dims, BF16)] * 2,
                *cost,
                rows,
                gate_weight,
                up_weight,
            )
        got = swap(send, "dp", n_dp, 1)
        folded.append(
            (keep, got, call(fold_body, shape(dims, BF16), total * width, 6 * total * width, keep, got))
        )
    value = []
    for c, (low, high) in enumerate(spans):
        keep, pair, send = folded[c]
        got = swap(send, "dp", n_dp, 2)
        mine = call(
            hidden_body, shape(send.shape[1:], BF16), total * width, 3 * total * width, keep, pair, got
        )
        beside = swap(mine, "dp", n_dp, 1)
        cost = 2 * total * (high - low) * out_width, 2 * (high - low) * out_width
        last = c == len(spans) - 1
        value = call(
            functools.partial(last_body, n_tp, low, high) if last else functools.partial(down_body, low, high),
            [shape((MOST, out_width), F32)] + [shape((MOST, out_width), BF16)] * (n_tp - 1)
            if last
            else [shape((total, out_width), F32)],
            *cost,
            mine,
            beside,
            down_weight,
            *value,
            scratch=[pltpu.VMEM((total, out_width), F32)] if last else (),
        )
    own, *sends = value
    got = []
    for q, send in enumerate(sends):
        got.append(swap(send, "tp", n_tp, q + 1))
    dims = (count, out_width)
    return call(
        final_body,
        shape(dims, BF16),
        2 * tokens.size,
        4 * tokens.size,
        spot,
        combine,
        own,
        *got,
        scratch=[pltpu.VMEM(dims, BF16), pltpu.SemaphoreType.DMA((PIECES,))],
        out_spec=pl.BlockSpec(memory_space=pltpu.HBM),
    )


def general(tokens, gate_weight, up_weight, down_weight, expert_ids, route_weights):
    held_mask = expert_ids == 0
    combine = jnp.sum(jnp.where(held_mask, route_weights, jnp.zeros_like(route_weights)), axis=1)
    hidden_width = gate_weight.shape[1]
    routed = jnp.any(held_mask, axis=1)
    slot_rank = jnp.cumsum(routed.astype(jnp.int32)) - 1
    slot_ids = jnp.arange(MOST, dtype=jnp.int32)
    dispatch = ((slot_rank[None, :] == slot_ids[:, None]) & routed[None, :]).astype(BF16)
    packed = jnp.dot(dispatch, tokens, preferred_element_type=F32).astype(BF16)
    row_block = lax.all_gather(packed, "tp", axis=0, tiled=True)
    gate_part = jnp.dot(row_block, gate_weight, preferred_element_type=F32).astype(BF16)
    up_part = jnp.dot(row_block, up_weight, preferred_element_type=F32).astype(BF16)
    gate_up = jnp.concatenate([gate_part, up_part], axis=1)
    summed = lax.psum(gate_up, "dp").astype(F32)
    hidden = (jax.nn.silu(summed[:, :hidden_width]) * summed[:, hidden_width:]).astype(BF16)
    partial_value = jnp.dot(hidden, down_weight, preferred_element_type=F32)
    result = jnp.dot(
        dispatch.T.astype(F32),
        lax.psum_scatter(
            partial_value.astype(BF16), "tp", scatter_dimension=0, tiled=True
        ).astype(F32),
        precision=lax.Precision.HIGHEST,
    )
    return (combine[:, None] * result).astype(BF16)


def solution(mesh):
    n_dp, n_tp = mesh.shape["dp"], mesh.shape["tp"]
    in_specs = (
        P(("groups", "tp"), "dp"),
        P("dp", "tp"),
        P("dp", "tp"),
        P("tp", "dp"),
        P(("groups", "tp"), None),
        P(("groups", "tp"), None),
    )
    out_specs = P(("groups", "tp"), "dp")
    def specialised(*args):
        return direct(n_dp, n_tp, *args)

    fits = n_dp == 4 and n_tp in (2, 4, 8)
    return jax.shard_map(
        specialised if fits else general,
        mesh=mesh,
        in_specs=in_specs,
        out_specs=out_specs,
        check_vma=False,
    )
```
